32 devices in a mesh: grp: 16 (over z, y, core), tp: 2 (over x).
Axes of the slice: x: 2, y: 2, z: 4, core: 2. Of those that a mesh axis runs over, the one named last changes fastest.
Arguments:
- tokens: bfloat16 [1024, 6144], P('grp', 'tp'), may hold values from -6 to 6
- norm_gain: float32 [6144], replicated, may hold values from 0.25 to 1.75
- router_weight: bfloat16 [6144, 8], replicated, may hold values from -0.078125 to 0.078125
- expert_ids: int32 [1024, 2], P('grp'), may hold values from 0 to 7, all different within a row; in each aligned block of 64 rows (0 to 63, 64 to 127, ...) at most 18 rows name the same one
- gate_proj: bfloat16 [6144, 65536], P(None, ('grp', 'tp')), may hold values from -0.078125 to 0.078125
- up_proj: bfloat16 [6144, 65536], P(None, ('grp', 'tp')), may hold values from -0.078125 to 0.078125
- down_proj: bfloat16 [65536, 6144], P(('grp', 'tp')), may hold values from -0.125 to 0.125
Outputs:
- mixed: bfloat16 [1024, 6144], P('grp', 'tp')
The draws below stay inside these ranges and needn't reach their ends.
Inputs may be any that keep to these rules, and one draw needn't show every extreme that they name: `expert_ids`: each row names two different experts; within the rows of one group (aligned blocks of 64 rows) no expert is named more than 18 times, and in some group one expert is named exactly 18 times.
All inputs are finite; a program needn't handle non-finite values.
Results may differ from the reference program's by a relative error of at most 0.017.
Values may be sent and summed in bfloat16 or wider, within the bound.
A program may use at most 128 MiB of HBM per device.

```python
import math
import jax
import jax.numpy as jnp
import numpy as np
from jax import lax

D = 6144
EXPERTS = 8
FF = 8192
TOK_GRP = 64
CAP = 18
TOKENS = 1024
N_GRP = 16
N_TP = 2


def with_spikes(values, own_key, source, target, blocks, factor):
    def block_of(axis_at):
        return (jnp.arange(values.shape[axis_at]) // (values.shape[axis_at] // blocks)).reshape((-1,) + (1,) * (values.ndim - 1 - axis_at))

    first = jax.random.permutation(own_key, blocks)[block_of(target)]
    far = (block_of(target) + blocks // 2) % blocks
    return jnp.where((block_of(source) == first) | (block_of(source) == far), factor * values, values)


def levels(stream_key, dims, shards, low, top_value):
    def one(axis_at, blocks):
        steps = jax.random.uniform(jax.random.fold_in(jax.random.fold_in(stream_key, 6), axis_at), (blocks,), jnp.float32, low / len(shards), top_value / len(shards))
        return jnp.repeat(jnp.exp(steps), dims[axis_at] // blocks).reshape((-1,) + (1,) * (len(dims) - axis_at - 1))

    factor_of = one(*shards[0])
    for cut in shards[1:]:
        factor_of = factor_of * one(*cut)
    return factor_of


def deal_out(own_key, own, number, rows, amount, top, limit, skew):
    order = jax.random.permutation(own_key, amount)
    crowded, ordinary = shares(amount, rows * top, limit, skew, True), shares(amount, rows * top, limit, skew, False)
    places = jnp.arange(amount)

    def named(sizes, turn):
        used = int((sizes > 0).sum())
        fixed = max(1, used // 4)
        moved = fixed + (places - fixed + turn * (used - fixed)) % max(1, amount - fixed)
        return jnp.zeros((amount,), jnp.int32).at[order[jnp.where(places < fixed, places, moved)]].set(jnp.asarray(sizes, jnp.int32))

    sizes = jnp.where(number % 4 == 0, named(crowded, number // 4), named(ordinary, number - number // 4 - 1))
    mixed = jax.random.permutation(jax.random.fold_in(own, 3), amount)
    giver, sink = mixed[0:amount // 2 * 2:2], mixed[1:amount // 2 * 2:2]
    margin = jnp.minimum(sizes[giver] - 1, limit - sizes[sink]) // 2
    margin = jnp.where((giver == order[0]) | (sink == order[0]) | (sizes[sink] == 0), 0, jnp.maximum(margin, 0))
    moved = jax.random.randint(jax.random.fold_in(own, 4), (amount // 2,), 0, 1 << 20) % (margin + 1)
    sizes = sizes.at[giver].add(-moved).at[sink].add(moved)
    labels = jnp.searchsorted(jnp.cumsum(sizes), jnp.arange(rows * top), side="right").astype(jnp.int32)
    table = labels.reshape(top, rows).T
    table = table[jax.random.permutation(jax.random.fold_in(own, 1), rows)]
    turn = jax.random.randint(jax.random.fold_in(own, 2), (rows, 1), 0, top)
    return jnp.take_along_axis(table, (jnp.arange(top)[None, :] + turn) % top, axis=1)


def shares(amount, total, most, slope, full):
    loads = [(1 << 20) // math.isqrt(standing ** slope) + 1 for standing in range(1, amount + 1)]
    largest = most if full else min(most, max(-(-total // amount), total * loads[0] // sum(loads)))
    least = 1 if total - largest >= amount - 1 else 0
    holding, surplus = [largest] + [least] * (amount - 1), total - largest - least * (amount - 1)
    while surplus > 0:
        candidates = [i for i in range(1, amount) if holding[i] < largest] or [i for i in range(1, amount) if holding[i] < most]
        whole, left = sum([loads[i] for i in candidates]), surplus
        for i in candidates:
            more = min(most - holding[i], max(1, left * loads[i] // whole), surplus)
            holding[i] = holding[i] + more
            surplus = surplus - more
    return np.array(holding)


def gaussian(key, shape, spread, bound, cuts=(), held_as=jnp.bfloat16):
    entries = jax.random.normal(key, shape, jnp.float32) * spread
    if len(cuts) > 0:
        entries = levels(key, shape, cuts, -0.22, 0.18) * entries
    return jnp.clip(entries, min=-bound, max=bound).astype(held_as)


def gaussian_with(rng, extent, width, most, split, heavy, held_as=jnp.bfloat16):
    drawn = width * jax.random.normal(rng, extent, jnp.float32)
    if split:
        drawn = drawn * levels(rng, extent, split, -0.22, 0.18)
    return jnp.clip(with_spikes(drawn, jax.random.fold_in(rng, 3), *heavy), -most, most).astype(held_as)


def setup_inputs(seed: int = 0) -> dict:
    streams_of = jax.random.split(jax.random.key(seed), 8)
    tokens = gaussian(streams_of[0], (TOKENS, D), 1.0, 6.0, ((0, 16), (1, 2)))
    norm_gain = jnp.clip(1.0 + 0.15 * jax.random.normal(streams_of[1], (D,), jnp.float32), 0.25, 1.75)
    router_weight = gaussian(streams_of[2], (D, EXPERTS), D ** -0.5, 0.078125)
    expert_ids_keys = jax.random.split(jax.random.fold_in(streams_of[3], 1), TOKENS // TOK_GRP)
    expert_ids_turns = jax.random.permutation(jax.random.fold_in(streams_of[3], 3), TOKENS // TOK_GRP)
    expert_ids = jax.vmap(lambda own, number: deal_out(jax.random.fold_in(streams_of[3], 2), own, number, TOK_GRP, EXPERTS, 2, CAP, 1))(expert_ids_keys, expert_ids_turns).reshape((TOKENS, 2))
    gate_proj = gaussian(streams_of[4], (D, EXPERTS * FF), D ** -0.5, 0.078125, ((1, 32),))
    up_proj = gaussian(streams_of[5], (D, EXPERTS * FF), D ** -0.5, 0.078125, ((1, 32),))
    down_proj = gaussian_with(streams_of[6], (EXPERTS * FF, D), FF ** -0.5, 0.125, ((0, 32),), (0, 1, 32, 2.75))
    return dict(tokens=tokens, norm_gain=norm_gain, router_weight=router_weight, expert_ids=expert_ids, gate_proj=gate_proj, up_proj=up_proj, down_proj=down_proj)


def reference(tokens, norm_gain, router_weight, expert_ids, gate_proj, up_proj, down_proj):
    epsilon = 1e-05
    values = tokens.astype(jnp.float32)
    mean_square = lax.optimization_barrier(jnp.mean(values * values, axis=-1, keepdims=True))
    normed = (values * lax.rsqrt(mean_square + epsilon) * norm_gain).astype(jnp.bfloat16)
    logits = jnp.dot(normed, router_weight, preferred_element_type=jnp.float32)
    chosen = jnp.take_along_axis(logits, expert_ids, axis=1)
    gate_first = 1.0 / (1.0 + jnp.exp(chosen[:, 1] - chosen[:, 0]))
    gate_second = 1.0 / (1.0 + jnp.exp(chosen[:, 0] - chosen[:, 1]))
    gates = jnp.stack([gate_first, gate_second], axis=1)
    owners = N_GRP // EXPERTS
    slice_width = FF // (owners * N_TP)
    group_ids = expert_ids.reshape(N_GRP, TOK_GRP, 2)
    group_gates = gates.reshape(N_GRP, TOK_GRP, 2)
    mixed = jnp.zeros((TOKENS, D), jnp.float32)
    for expert in range(EXPERTS):
        hits = (group_ids == expert).astype(jnp.int32)
        routed = lax.optimization_barrier(jnp.sum(hits, axis=-1))
        gate_table = lax.optimization_barrier(jnp.sum(group_gates * hits.astype(jnp.float32), axis=-1))
        order = jnp.argsort(1 - routed, axis=1, stable=True)[:, :CAP].astype(jnp.int32)
        valid = jnp.take_along_axis(routed, order, axis=1).astype(jnp.float32)
        token_index = (order + jnp.arange(N_GRP, dtype=jnp.int32)[:, None] * TOK_GRP).reshape(-1)
        row_weight = (jnp.take_along_axis(gate_table, order, axis=1) * valid).reshape(-1)
        row_block = normed[token_index]
        total = jnp.zeros((N_GRP * CAP, D), jnp.float32)
        for quarter in range(owners):
            quarter_sum = jnp.zeros((N_GRP * CAP, D), jnp.float32)
            for piece in range(N_TP):
                column = expert * FF + (quarter * N_TP + piece) * slice_width
                gate_act = jnp.dot(row_block, gate_proj[:, column:column + slice_width], preferred_element_type=jnp.float32)
                up_act = jnp.dot(row_block, up_proj[:, column:column + slice_width], preferred_element_type=jnp.float32)
                hidden = (jax.nn.silu(gate_act) * up_act).astype(jnp.bfloat16)
                partial_out = jnp.dot(hidden, down_proj[column:column + slice_width], preferred_element_type=jnp.float32).astype(jnp.bfloat16)
                quarter_sum = quarter_sum + lax.optimization_barrier(partial_out).astype(jnp.float32)
            total = total + lax.optimization_barrier(quarter_sum.astype(jnp.bfloat16)).astype(jnp.float32)
        mixed = mixed.at[token_index].add(total * row_weight[:, None])
    return mixed.astype(jnp.bfloat16)
```

```python
from functools import partial

import jax
import jax.numpy as jnp
from jax import lax
from jax.experimental import pallas as pl
from jax.experimental.pallas import tpu as pltpu
from jax.sharding import PartitionSpec as P

CAP = 18
MESH = pl.DeviceIdType.MESH


epsilon = 1e-05


def place(experts, owners, pieces):
    g, p = lax.axis_index("grp"), lax.axis_index("tp")
    return g, p, g // owners, lax.rem(g, owners)


def greet(experts, owners, pieces):
    g, p, c, k = place(experts, owners, pieces)
    barrier = pltpu.get_barrier_semaphore()
    peers = [(lax.rem(c + j, experts) * owners + k, p) for j in range(1, experts)]
    peers += [(c * owners + lax.rem(k + d, owners), p) for d in range(1, owners)]
    peers += [(g, lax.rem(p + t, pieces)) for t in range(1, pieces)]
    for peer in peers:
        pl.semaphore_signal(barrier, inc=1, device_id=peer, device_id_type=MESH)
    pl.semaphore_wait(barrier, len(peers))


def remote(src, dst, sems, index, peer):
    return pltpu.make_async_remote_copy(
        src_ref=src,
        dst_ref=dst,
        send_sem=sems.at[(0,) + index],
        recv_sem=sems.at[(1,) + index],
        device_id=peer,
        device_id_type=MESH,
    )


def slabs_of(experts, owners, pieces, capacity, width):
    for t in range(pieces):
        for s in range(experts):
            for o in range(owners):
                rows = pl.ds((s * owners + o) * capacity, capacity)
                yield (t, s, o), (rows, pl.ds(t * width, width))


def dispatch_kernel(
    experts, owners, pieces, src, rows_out, out, local, direct, core, cross, cross_core
):
    g, p, c, k = place(experts, owners, pieces)
    greet(experts, owners, pieces)
    keep = pltpu.make_async_copy(src.at[c], out.at[p, c, k], local)
    keep.start()
    sends = {}
    for j in range(1, experts):
        e = lax.rem(c + j, experts)
        sends[j] = remote(src.at[e], out.at[p, c, k], direct, (j,), (e * owners + k, p))
        sends[j].start()
    to_core, to_piece, to_cross = [], {}, []
    for j in range(experts):
        s = lax.rem(c + experts - j, experts)
        if j == 0:
            keep.wait()
        else:
            sends[j].wait_recv()
        slab = out.at[p, s, k]
        for t in range(1, pieces):
            copy = remote(slab, slab, cross, (t, j), (g, lax.rem(p + t, pieces)))
            copy.start()
            to_piece[t, j] = copy
        for d in range(1, owners):
            peer = (c * owners + lax.rem(k + d, owners), p)
            copy = remote(slab, slab, core, (d, j), peer)
            copy.start()
            to_core.append(copy)
    for j in range(experts):
        s = lax.rem(c + experts - j, experts)
        for t in range(1, pieces):
            to_piece[t, j].wait_recv()
            slab = out.at[lax.rem(p + pieces - t, pieces), s, k]
            for d in range(1, owners):
                peer = (c * owners + lax.rem(k + d, owners), p)
                copy = remote(slab, slab, cross_core, (t, d, j), peer)
                copy.start()
                to_cross.append(copy)
    for copy in to_core + to_cross:
        copy.wait()
    for copy in list(sends.values()) + list(to_piece.values()):
        copy.wait_send()
    for slab, block in slabs_of(experts, owners, pieces, *src.shape[1:]):
        rows_out[block] = out[slab]


def collect_kernel(
    experts, owners, pieces, rows_in, out, part, near, leaving, arrived, final, core, cross, back
):
    g, p, c, k = place(experts, owners, pieces)
    greet(experts, owners, pieces)
    order = list(range(1, experts)) + [0]
    near_copies, cross_copies, back_copies = {}, {}, {}
    for slab, block in slabs_of(experts, owners, pieces, *out.shape[1:]):
        part[slab] = rows_in[block]
    for t in list(range(1, pieces)) + [0]:
        for j in order:
            s = lax.rem(c + j, experts)
            piece = lax.rem(p + t, pieces)
            for d in range(1, owners):
                other = lax.rem(k + d, owners)
                copy = remote(
                    part.at[piece, s, other],
                    near.at[d - 1, t, j],
                    core,
                    (d, t, j),
                    (c * owners + other, p),
                )
                copy.start()
                near_copies[d, t, j] = copy

    def chip_sum(t, j):
        total = part[lax.rem(p + t, pieces), lax.rem(c + j, experts), k].astype(jnp.float32)
        for d in range(1, owners):
            near_copies[d, t, j].wait_recv()
            total = total + near[d - 1, t, j].astype(jnp.float32)
        return total

    for j in order:
        for t in range(1, pieces):
            leaving[t - 1, j] = chip_sum(t, j).astype(leaving.dtype)
            copy = remote(
                leaving.at[t - 1, j],
                arrived.at[t - 1, j],
                cross,
                (t, j),
                (g, lax.rem(p + t, pieces)),
            )
            copy.start()
            cross_copies[t, j] = copy
    for j in order:
        total = chip_sum(0, j)
        for t in range(1, pieces):
            cross_copies[t, j].wait_recv()
            total = total + arrived[t - 1, j].astype(jnp.float32)
        if j == 0:
            out[c] = total.astype(out.dtype)
        else:
            final[j] = total.astype(final.dtype)
            peer = (lax.rem(c + j, experts) * owners + k, p)
            copy = remote(final.at[j], out.at[c], back, (j,), peer)
            copy.start()
            back_copies[j] = copy
    for copy in back_copies.values():
        copy.wait()
    for copy in list(near_copies.values()) + list(cross_copies.values()):
        copy.wait_send()


def dispatch(outgoing, owners, pieces):
    experts, capacity, width = outgoing.shape
    dma = pltpu.SemaphoreType.DMA
    return pl.pallas_call(
        partial(dispatch_kernel, experts, owners, pieces),
        out_shape=jax.ShapeDtypeStruct(
            (experts * owners * capacity, pieces * width), outgoing.dtype
        ),
        in_specs=[pl.BlockSpec(memory_space=pltpu.VMEM)],
        out_specs=pl.BlockSpec(memory_space=pltpu.VMEM),
        scratch_shapes=[
            pltpu.VMEM((pieces, experts, owners, capacity, width), outgoing.dtype),
            dma,
            dma((2, experts)),
            dma((2, owners, experts)),
            dma((2, pieces, experts)),
            dma((2, pieces, owners, experts)),
        ],
        compiler_params=pltpu.CompilerParams(
            collective_id=0, has_side_effects=True, vmem_limit_bytes=60 * 2**20
        ),
    )(outgoing)


def collect(part, experts, owners, pieces):
    capacity, width = part.shape[0] // (experts * owners), part.shape[1] // pieces
    dma = pltpu.SemaphoreType.DMA
    slabs = lambda *lead: pltpu.VMEM(lead + (capacity, width), part.dtype)
    return pl.pallas_call(
        partial(collect_kernel, experts, owners, pieces),
        out_shape=jax.ShapeDtypeStruct((experts, capacity, width), part.dtype),
        in_specs=[pl.BlockSpec(memory_space=pltpu.VMEM)],
        out_specs=pl.BlockSpec(memory_space=pltpu.VMEM),
        scratch_shapes=[
            slabs(pieces, experts, owners),
            slabs(max(owners - 1, 1), pieces, experts),
            slabs(max(pieces - 1, 1), experts),
            slabs(max(pieces - 1, 1), experts),
            slabs(experts),
            dma((2, owners, pieces, experts)),
            dma((2, pieces, experts)),
            dma((2, experts)),
        ],
        compiler_params=pltpu.CompilerParams(
            collective_id=1, has_side_effects=True, vmem_limit_bytes=60 * 2**20
        ),
    )(part)


def per_device(tokens, norm_gain, router_weight, expert_ids, gate_proj, up_proj, down_proj):
    tok_rows, local_width = tokens.shape
    experts = router_weight.shape[1]
    groups, pieces = lax.axis_size("grp"), lax.axis_size("tp")
    owners = groups // experts
    capacity = CAP
    start = lax.axis_index("tp") * local_width
    gain = lax.dynamic_slice_in_dim(norm_gain, start, local_width)
    router = lax.dynamic_slice_in_dim(router_weight, start, local_width, axis=0)
    values = tokens.astype(jnp.float32)
    squares = jnp.sum(values * values, axis=-1)
    squares = jnp.sum(lax.all_gather(squares, "tp"), axis=0)
    mean_square = (squares / (local_width * pieces))[:, None]
    normed = (values * lax.rsqrt(mean_square + epsilon) * gain).astype(jnp.bfloat16)
    logits = jnp.dot(normed, router, preferred_element_type=jnp.float32)
    logits = jnp.sum(lax.all_gather(logits, "tp"), axis=0)
    expert_iota = jnp.arange(experts, dtype=jnp.int32)[None, :]
    chosen_first = (expert_ids[:, 0:1] == expert_iota).astype(jnp.int32)
    chosen_second = (expert_ids[:, 1:2] == expert_iota).astype(jnp.int32)
    first_logit = jnp.sum(logits * chosen_first.astype(jnp.float32), axis=-1)
    second = jnp.sum(logits * chosen_second.astype(jnp.float32), axis=-1)
    gate_first = 1.0 / (1.0 + jnp.exp(second - first_logit))
    gate_second = 1.0 / (1.0 + jnp.exp(first_logit - second))
    gate_table = gate_first[:, None] * chosen_first.astype(jnp.float32) + gate_second[
        :, None
    ] * chosen_second.astype(jnp.float32)
    routed = chosen_first + chosen_second
    slot_index = jnp.cumsum(routed, axis=0) - 1
    slot_iota = jnp.arange(capacity, dtype=jnp.int32)
    slot_picks = (slot_index.T[:, None, :] == slot_iota[None, :, None]) & (
        routed.T[:, None, :] == 1
    )
    selector = slot_picks.astype(jnp.bfloat16)
    outgoing = jnp.einsum(
        "ect,td->ecd", selector, normed, preferred_element_type=jnp.float32
    ).astype(jnp.bfloat16)
    row_block = dispatch(outgoing, owners, pieces)
    gate_act = jnp.dot(row_block, gate_proj, preferred_element_type=jnp.float32)
    up_act = jnp.dot(row_block, up_proj, preferred_element_type=jnp.float32)
    hidden = (jax.nn.silu(gate_act) * up_act).astype(jnp.bfloat16)
    partial_out = jnp.dot(hidden, down_proj, preferred_element_type=jnp.float32).astype(
        jnp.bfloat16
    )
    summed = collect(partial_out, experts, owners, pieces).astype(jnp.float32)
    combine = slot_picks.astype(jnp.float32) * gate_table.T[:, None, :]
    mixed = jnp.einsum("ect,ecd->td", combine, summed, precision=lax.Precision.HIGHEST)
    return mixed.astype(jnp.bfloat16)


def solution(mesh):
    in_specs = (
        P("grp", "tp"),
        P(),
        P(),
        P("grp", None),
        P(None, ("grp", "tp")),
        P(None, ("grp", "tp")),
        P(("grp", "tp"), None),
    )
    out_specs = P("grp", "tp")
    return jax.shard_map(
        per_device, mesh=mesh, in_specs=in_specs, out_specs=out_specs, check_vma=False
    )
```
